32 devices in a mesh: bank: 8 (over z, y), ens: 4 (over x, core).
Axes of the slice: x: 2, y: 2, z: 4, core: 2. Of those that a mesh axis runs over, the one named last changes fastest.
Arguments:
- item_ids: int32 [1024, 2], P(('ens', 'bank')), parts along dimension 0, may hold values from 0 to 2047
- large_table: bfloat16 [8192, 256], P(('ens', 'bank')), parts along dimension 0, may hold values from -6 to 6
- dense_part: float32 [1024, 256], P(('ens', 'bank')), parts along dimension 0, may hold values from -6 to 6
- small_ids: int32 [1024], P(('ens', 'bank')), parts along dimension 0, may hold values from 0 to 15
- small_table: bfloat16 [64, 256], P(('ens', 'bank')), parts along dimension 0, may hold values from -6 to 6
- scale_ids: int32 [1024], P(('ens', 'bank')), parts along dimension 0, may hold values from 0 to 15
Outputs:
- features: float32 [1024, 256], P(('ens', 'bank')), parts along dimension 0
The draws below stay inside these ranges and needn't reach their ends.
There are 4 independent parts, one for each index of `ens`. The reference program is written for one: setup_inputs(seed, part) draws one part's arguments, and reference() takes and returns one part's arrays. A program takes and returns all parts, laid end to end along the dimension named above; each array names one. Nothing has to cross between parts.
All inputs are finite; a program needn't handle non-finite values.
Results may differ from the reference program's by a relative error of at most 0.0003.
Values may be sent and summed in bfloat16 or wider, within the bound.
No kernel may reach another device: no remote copies, remote signals or barrier semaphores. Data moves between devices by JAX's collectives and lax.ppermute only.
A program may use at most 64 MiB of HBM per device.

```python
import math
import jax
import jax.numpy as jnp
import numpy as np
from jax import lax

EXAMPLES = 256
FEATURES = 256
PICKS = 2
BIG_ROWS = 2048
SMALL_ROWS = 16


def place_ends(result, own_key, least, high):
    dims = result.shape
    index_at = [jax.random.randint(jax.random.fold_in(own_key, axis), (), 0, dims[axis]) for axis in range(len(dims))]
    result = result.at[tuple(index_at)].set(least)
    longest = dims.index(max(dims))
    index_at[longest] = (index_at[longest] + 1) % dims[longest]
    return result.at[tuple(index_at)].set(high)


def steps_of(own_key, dims, cuts, smallest, largest):
    level = 1.0
    for dim, shards_of in cuts:
        steps = jax.random.uniform(jax.random.fold_in(jax.random.fold_in(own_key, 6), dim), (shards_of,), jnp.float32, smallest / len(cuts), largest / len(cuts))
        level = level * jnp.repeat(jnp.exp(steps), dims[dim] // shards_of).reshape((-1,) + (1,) * (len(dims) - 1 - dim))
    return level


def rank_table(number_of, skew):
    loads = [(1 << 20) // math.isqrt(grade ** skew) + 1 for grade in range(1, number_of + 1)]
    scale = 1 + sum(loads) // (1 << 30)
    return np.cumsum(np.array([max(1, weight // scale) for weight in loads]))


def ranked_ids(own_key, extent, number_of, skew):
    grid = rank_table(number_of, skew)
    ticket = jax.random.randint(jax.random.fold_in(own_key, 1), extent, 0, int(grid[number_of - 1]))
    standing = jnp.searchsorted(jnp.asarray(grid, jnp.int32), ticket, side="right")
    return jax.random.permutation(jax.random.fold_in(own_key, 2), number_of)[standing].astype(jnp.int32)


def gaussian(stream_key, dims, spread, bound, cuts=(), kind=jnp.bfloat16):
    factor_of = steps_of(stream_key, dims, cuts, -0.22, 0.18) if cuts else 1.0
    values = jax.random.normal(stream_key, dims, jnp.float32) * spread * factor_of
    return jnp.minimum(jnp.maximum(values, -bound), bound).astype(kind)


def setup_inputs(seed: int = 0, part: int = 0) -> dict:
    seeds = jax.random.split(jax.random.key(seed), 7)
    part_keys = jax.random.split(jax.random.fold_in(seeds[6], part), 7)
    item_ids = place_ends(ranked_ids(part_keys[0], (EXAMPLES, PICKS), BIG_ROWS, 1), jax.random.fold_in(part_keys[0], 3), 0, BIG_ROWS - 1).astype(jnp.int32)
    large_table = gaussian(part_keys[1], (BIG_ROWS, FEATURES), 1.0, 6.0, ((0, 8),))
    dense_part = gaussian(part_keys[2], (EXAMPLES, FEATURES), 1.0, 6.0, ((0, 8),), jnp.float32)
    small_ids = place_ends(jax.random.randint(part_keys[3], (EXAMPLES,), 0, SMALL_ROWS), jax.random.fold_in(part_keys[3], 1), 0, SMALL_ROWS - 1).astype(jnp.int32)
    small_table = gaussian(part_keys[4], (SMALL_ROWS, FEATURES), 1.0, 6.0, ((0, 8),))
    scale_ids = place_ends(ranked_ids(part_keys[5], (EXAMPLES,), SMALL_ROWS, 1), jax.random.fold_in(part_keys[5], 3), 0, SMALL_ROWS - 1).astype(jnp.int32)
    return {"item_ids": item_ids, "large_table": large_table, "dense_part": dense_part, "small_ids": small_ids, "small_table": small_table, "scale_ids": scale_ids}


def reference(item_ids, large_table, dense_part, small_ids, small_table, scale_ids):
    pooled = lax.optimization_barrier(jnp.sum(large_table[item_ids].astype(jnp.float32), axis=1)) * PICKS ** (-0.5)
    small_rows = small_table[small_ids].astype(jnp.float32)
    dense_part = dense_part * small_table[scale_ids].astype(jnp.float32)
    total = dense_part + pooled * small_rows
    features = total * lax.rsqrt(lax.optimization_barrier(jnp.mean(total * total, axis=-1, keepdims=True)) + 1e-06)
    return features
```

```python
import functools

import jax
import jax.numpy as jnp
from jax import lax
from jax.experimental import pallas as pl
from jax.experimental.pallas import tpu as pltpu
from jax.sharding import PartitionSpec as P

PICKS = 2


def partial_kernel(rows, device_ref, ids_ref, *refs):
    block_refs, out_ref = refs[:-1], refs[-1]
    examples = ids_ref.shape[0]
    small = block_refs[0].shape[0] - rows
    ids = ids_ref[...]
    place = lax.broadcasted_iota(jnp.int32, (examples, rows), 1)
    pooled = jnp.zeros((examples, out_ref.shape[1]), jnp.float32)
    for k, block_ref in enumerate(block_refs):
        local = ids - (device_ref[0] ^ k) * rows
        counts = jnp.zeros((examples, rows), jnp.float32)
        for pick in range(ids.shape[1]):
            counts += jnp.where(place == local[:, pick : pick + 1], 1.0, 0.0)
        pooled += jnp.dot(
            counts.astype(jnp.bfloat16), block_ref[:rows, :], preferred_element_type=jnp.float32
        )
        out_ref[examples + k * small : examples + (k + 1) * small, :] = block_ref[rows:, :].astype(
            jnp.float32
        )
    out_ref[:examples, :] = pooled


def finish_kernel(small, block, bank, device_ref, dense_ref, small_ids_ref, scale_ids_ref, *refs):
    part_refs, out_ref = refs[:-1], refs[-1]
    examples = dense_ref.shape[0]
    slot = lax.broadcasted_iota(jnp.int32, (block * small, examples), 0)
    pooled = jnp.zeros(dense_ref.shape, jnp.float32)
    small_rows = jnp.zeros(dense_ref.shape, jnp.float32)
    scale_rows = jnp.zeros(dense_ref.shape, jnp.float32)
    small_ids = small_ids_ref[...]
    scale_ids = scale_ids_ref[...]
    for d, part_ref in enumerate(part_refs):
        pooled += part_ref[:examples, :]
        table = part_ref[examples:, :].astype(jnp.bfloat16)
        owner = (device_ref[0] + d * block) & (bank - 1)
        row = (owner ^ (slot // small)) * small + slot % small
        pick = lambda ids: lax.dot_general(
            jnp.where(row == ids, 1.0, 0.0).astype(jnp.bfloat16),
            table,
            (((0,), (0,)), ((), ())),
            preferred_element_type=jnp.float32,
        )
        small_rows += pick(small_ids)
        scale_rows += pick(scale_ids)
    total = dense_ref[...] * scale_rows + pooled * PICKS ** (-0.5) * small_rows
    power = jnp.mean(total * total, axis=-1, keepdims=True)
    out_ref[...] = total * lax.rsqrt(power + 1e-06)


def shards(bank, item_ids, large_table, dense_part, small_ids, small_table, scale_ids):
    block = next(size for size in (4, 2, 1) if bank % size == 0)
    rows, features = large_table.shape
    small = small_table.shape[0]
    examples = item_ids.shape[0]
    device = lax.axis_index("bank").astype(jnp.int32).reshape(1)
    steps = range(1, bank // block)
    smem = pl.BlockSpec(memory_space=pltpu.SMEM)
    vmem = pl.BlockSpec(memory_space=pltpu.VMEM)

    asked = [item_ids] + [
        lax.ppermute(item_ids, "bank", [(i, (i + d * block) % bank) for i in range(bank)])
        for d in steps
    ]
    own = jnp.concatenate([large_table, small_table], axis=0)
    blocks = [own] + [
        lax.ppermute(own, "bank", [(i, i ^ k) for i in range(bank)]) for k in range(1, block)
    ]

    def partial(ids):
        return pl.pallas_call(
            functools.partial(partial_kernel, rows),
            out_shape=jax.ShapeDtypeStruct((examples + block * small, features), jnp.float32),
            in_specs=[smem] + [vmem] * (1 + block),
            out_specs=vmem,
        )(device, ids, *blocks)

    answers = [
        lax.ppermute(partial(asked[d]), "bank", [(i, (i - d * block) % bank) for i in range(bank)])
        for d in steps
    ]
    parts = [partial(item_ids)] + answers
    return pl.pallas_call(
        functools.partial(finish_kernel, small, block, bank),
        out_shape=jax.ShapeDtypeStruct((examples, features), jnp.float32),
        in_specs=[smem] + [vmem] * (3 + len(parts)),
        out_specs=vmem,
    )(device, dense_part, small_ids.reshape(1, -1), scale_ids.reshape(1, -1), *parts)


def solution(mesh):
    return jax.shard_map(
        functools.partial(shards, mesh.shape["bank"]),
        mesh=mesh,
        in_specs=(
            P(("ens", "bank"), None),
            P(("ens", "bank"), None),
            P(("ens", "bank"), None),
            P(("ens", "bank")),
            P(("ens", "bank"), None),
            P(("ens", "bank")),
        ),
        out_specs=P(("ens", "bank"), None),
        check_vma=False,
    )
```

```python
import functools

import jax
import jax.numpy as jnp
from jax import lax
from jax.experimental import pallas as pl
from jax.experimental.pallas import tpu as pltpu
from jax.sharding import PartitionSpec as P

PICKS = 2


def in_vmem(array):
    return pltpu.with_memory_space_constraint(array, pltpu.VMEM)


def partial_kernel(rows, block, device_ref, ids_ref, *refs):
    block_refs, passed = refs[:block], refs[block:]
    count = len(passed) // 2
    out_ref = passed[count]
    for from_ref, to_ref in zip(passed[:count], passed[count + 1 :]):
        to_ref[...] = from_ref[...]
    examples = ids_ref.shape[1]
    small = block_refs[0].shape[0] - rows
    ids = jnp.transpose(ids_ref[...])
    place = lax.broadcasted_iota(jnp.int32, (examples, rows), 1)
    pooled = jnp.zeros((examples, out_ref.shape[1]), jnp.float32)
    for k, block_ref in enumerate(block_refs):
        local = ids - (device_ref[0] ^ k) * rows
        counts = jnp.zeros((examples, rows), jnp.float32)
        for pick in range(ids.shape[1]):
            counts += jnp.where(place == local[:, pick : pick + 1], 1.0, 0.0)
        pooled += jnp.dot(
            counts.astype(jnp.bfloat16), block_ref[:rows, :], preferred_element_type=jnp.float32
        )
        out_ref[examples + k * small : examples + (k + 1) * small, :] = block_ref[rows:, :].astype(
            jnp.float32
        )
    out_ref[:examples, :] = pooled


def finish_kernel(small, block, bank, device_ref, dense_ref, small_ids_ref, scale_ids_ref, *refs):
    part_refs, out_ref = refs[:-1], refs[-1]
    examples = dense_ref.shape[0]
    slot = lax.broadcasted_iota(jnp.int32, (block * small, examples), 0)
    pooled = jnp.zeros(dense_ref.shape, jnp.float32)
    small_rows = jnp.zeros(dense_ref.shape, jnp.float32)
    scale_rows = jnp.zeros(dense_ref.shape, jnp.float32)
    small_ids = small_ids_ref[...]
    scale_ids = scale_ids_ref[...]
    for d, part_ref in enumerate(part_refs):
        pooled += part_ref[:examples, :]
        table = part_ref[examples:, :].astype(jnp.bfloat16)
        owner = (device_ref[0] + d * block) & (bank - 1)
        row = (owner ^ (slot // small)) * small + slot % small
        pick = lambda ids: lax.dot_general(
            jnp.where(row == ids, 1.0, 0.0).astype(jnp.bfloat16),
            table,
            (((0,), (0,)), ((), ())),
            preferred_element_type=jnp.float32,
        )
        small_rows += pick(small_ids)
        scale_rows += pick(scale_ids)
    total = dense_ref[...] * scale_rows + pooled * PICKS ** (-0.5) * small_rows
    power = jnp.mean(total * total, axis=-1, keepdims=True)
    out_ref[...] = total * lax.rsqrt(power + 1e-06)


def shards(bank, item_ids, large_table, dense_part, small_ids, small_table, scale_ids):
    block = next(size for size in (4, 2, 1) if bank % size == 0)
    rows, features = large_table.shape
    small = small_table.shape[0]
    examples = item_ids.shape[0]
    item_ids = jnp.transpose(item_ids)
    device = lax.axis_index("bank").astype(jnp.int32).reshape(1)
    steps = range(1, bank // block)
    smem = pl.BlockSpec(memory_space=pltpu.SMEM)
    vmem = pl.BlockSpec(memory_space=pltpu.VMEM)

    asked = [item_ids] + [
        lax.ppermute(item_ids, "bank", [(i, (i + d * block) % bank) for i in range(bank)])
        for d in steps
    ]
    own = jnp.concatenate([large_table, small_table], axis=0)
    blocks = [own] + [
        lax.ppermute(own, "bank", [(i, i ^ k) for i in range(bank)]) for k in range(1, block)
    ]

    def partial(ids, *passed):
        return pl.pallas_call(
            functools.partial(partial_kernel, rows, block),
            out_shape=[pltpu.VMEM((examples + block * small, features), jnp.float32)]
            + [pltpu.VMEM(p.shape, p.dtype) for p in passed],
            in_specs=[smem] + [vmem] * (1 + block + len(passed)),
            out_specs=[vmem] * (1 + len(passed)),
        )(device, *map(in_vmem, [ids] + blocks + list(passed)))

    answers = [
        lax.ppermute(partial(asked[d])[0], "bank", [(i, (i - d * block) % bank) for i in range(bank)])
        for d in steps
    ]
    own_part, small_ids, scale_ids = partial(
        item_ids, small_ids.reshape(1, -1), scale_ids.reshape(1, -1)
    )
    parts = [own_part] + answers
    return pl.pallas_call(
        functools.partial(finish_kernel, small, block, bank),
        out_shape=jax.ShapeDtypeStruct((examples, features), jnp.float32),
        in_specs=[smem] + [vmem] * (3 + len(parts)),
        out_specs=vmem,
    )(
        device,
        *map(in_vmem, [dense_part, small_ids, scale_ids] + parts),
    )


def solution(mesh):
    return jax.shard_map(
        functools.partial(shards, mesh.shape["bank"]),
        mesh=mesh,
        in_specs=(
            P(("ens", "bank"), None),
            P(("ens", "bank"), None),
            P(("ens", "bank"), None),
            P(("ens", "bank")),
            P(("ens", "bank"), None),
            P(("ens", "bank")),
        ),
        out_specs=P(("ens", "bank"), None),
        check_vma=False,
    )
```
